32 devices in a mesh: kx: 8 (over z, x), cz: 4 (over y, core).
Axes of the slice: x: 2, y: 2, z: 4, core: 2. Of those that a mesh axis runs over, the one named last changes fastest.
Arguments:
- field_modes: bfloat16 [512, 4, 12288], P('cz', None, 'kx'), may hold values from -6 to 6
- cotangent: bfloat16 [512, 4, 12288], P('cz', None, 'kx'), may hold values from -6 to 6
Outputs:
- mode_gradient: bfloat16 [512, 4, 12288], P('cz', None, 'kx')
The draws below stay inside these ranges and needn't reach their ends.
All inputs are finite; a program needn't handle non-finite values.
Results may differ from the reference program's by a relative error of at most 0.009.
Values may be sent and summed in bfloat16 or wider, within the bound.
A program may use at most 128 MiB of HBM per device.

```python
import math
import jax
import jax.numpy as jnp
from jax import lax

FIELDS = 4
NZ = 512
MZ = 768
NX = 768
Y = 16


def steps_of(key, dims, pieces, smallest, largest):
    gain, own = 1.0, jax.random.fold_in(key, 6)
    for axis_at, shards_of in pieces:
        heights = jnp.exp(jax.random.uniform(jax.random.fold_in(own, axis_at), (shards_of,), jnp.float32, smallest / len(pieces), largest / len(pieces)))
        gain = gain * jnp.repeat(heights, dims[axis_at] // shards_of).reshape([-1 if axis == axis_at else 1 for axis in range(len(dims))])
    return gain


def normal_values(rng, shape, spread, bound, cuts=(), kind=jnp.bfloat16):
    factor_of = steps_of(rng, shape, cuts, -0.22, 0.18) if cuts else 1.0
    drawn = jax.random.normal(rng, shape, jnp.float32) * spread * factor_of
    return jnp.minimum(jnp.maximum(drawn, -bound), bound).astype(kind)


def setup_inputs(seed: int = 0) -> dict:
    key_of = jax.random.split(jax.random.key(seed), 3)
    return {
        "field_modes": normal_values(key_of[0], (NZ, FIELDS, NX * Y), 1.0, 6.0, ((0, 4), (2, 8))),
        "cotangent": normal_values(key_of[1], (NZ, FIELDS, NX * Y), 1.0, 6.0, ((0, 4), (2, 8))),
    }


def cosine_table():
    row_index = jnp.arange(MZ, dtype=jnp.int32)
    col_index = jnp.arange(NZ, dtype=jnp.int32)
    position = col_index[None, :] * (2 * row_index[:, None] + 1) % (4 * MZ)
    return jnp.cos(jnp.pi * position.astype(jnp.float32) / (2 * MZ))

def hartley_table():
    points = jnp.arange(NX, dtype=jnp.int32)
    position = points[:, None] * points[None, :] % NX
    phases = 2.0 * jnp.pi * position.astype(jnp.float32) / NX
    return ((jnp.cos(phases) + jnp.sin(phases)) / math.sqrt(NX)).astype(jnp.bfloat16)

def product_gradient(fields, adjoint):
    vertical = fields[2]
    return jnp.stack([adjoint[0] * vertical, adjoint[1] * vertical, adjoint[0] * fields[0] + adjoint[1] * fields[1] + 2.0 * adjoint[2] * vertical + adjoint[3] * fields[3], adjoint[3] * vertical]).astype(jnp.bfloat16)

def reference(field_modes, cotangent):
    highest = lax.Precision.HIGHEST
    field_grid = field_modes.reshape(NZ, FIELDS, NX, Y)
    cotangent_grid = cotangent.reshape(NZ, FIELDS, NX, Y)
    cosines = cosine_table()
    synthesis_full = (cosines * math.sqrt(2.0 / NZ)).astype(jnp.bfloat16).astype(jnp.float32)
    projection_full = (cosines * math.sqrt(2.0 / MZ)).astype(jnp.bfloat16).astype(jnp.float32)
    hartley_full = hartley_table().astype(jnp.float32)
    block_rows = 8
    block_count = Y // block_rows

    def one_block(position):
        first_row = position * block_rows
        mode_block = lax.dynamic_slice_in_dim(field_grid, first_row, block_rows, 3).astype(jnp.float32)
        adjoint_block = lax.dynamic_slice_in_dim(cotangent_grid, first_row, block_rows, 3).astype(jnp.float32)
        lifted_fields = jnp.einsum('zk,kfmy->fzmy', synthesis_full, mode_block, precision=highest).astype(jnp.bfloat16).astype(jnp.float32)
        lifted_adjoint = jnp.einsum('zk,kfmy->fzmy', projection_full, adjoint_block, precision=highest).astype(jnp.bfloat16).astype(jnp.float32)
        fields = jnp.einsum('xm,fzmy->fzxy', hartley_full, lifted_fields, precision=highest)
        adjoint = jnp.einsum('xm,fzmy->fzxy', hartley_full, lifted_adjoint, precision=highest)
        gradient = product_gradient(fields, adjoint).astype(jnp.float32)
        turned = jnp.einsum('xm,fzxy->fzmy', hartley_full, gradient, precision=highest).astype(jnp.bfloat16).astype(jnp.float32)
        spectral = jnp.einsum('zk,fzmy->kfmy', synthesis_full, turned, precision=highest)
        return spectral.astype(jnp.bfloat16)
    blocks = lax.map(one_block, jnp.arange(block_count, dtype=jnp.int32))
    return jnp.moveaxis(blocks, 0, 3).reshape(NZ, FIELDS, NX * Y)
```

```python
import functools
import math

import jax
import jax.numpy as jnp
import numpy as np
from jax import lax
from jax.experimental import pallas as pl
from jax.experimental.pallas import tpu as pltpu
from jax.sharding import PartitionSpec as P

MZ = 768
Y = 16
MESH = pl.DeviceIdType.MESH


def cosine_table(rows, columns):
    position = (np.arange(columns)[None, :] * (2 * np.arange(rows)[:, None] + 1)) % (4 * rows)
    return np.cos(np.pi * position / (2 * rows)).astype(np.float32)


def hartley_table(points):
    index = np.arange(points)
    phases = 2.0 * np.pi * ((index[:, None] * index[None, :]) % points) / points
    return (np.cos(phases) + np.sin(phases)) / math.sqrt(points)


def matmul(a, b):
    return jnp.dot(a, b, preferred_element_type=jnp.float32)


def kernel(
    nkx, ncz, shares,
    field_src, adjoint_src, hartley, lift_fields, lift_adjoint, lower,
    out,
    held, mixed, halves, lowered, turned, result,
    in_send, in_recv, swap_send, swap_recv, back_send, back_recv, out_send, out_recv,
):
    rows_y, fields, local_m, local_k = field_src.shape
    per_share = ncz // shares
    points_x = hartley.shape[0]
    share_x = points_x // shares
    i, j = lax.axis_index("kx"), lax.axis_index("cz")
    linear = i * ncz + j
    my_y, my_share = linear // shares, lax.rem(linear, shares)
    to_share = j // per_share
    my_part = lax.rem(j, per_share)
    my_slot = i * per_share + my_part
    stays = to_share == my_share

    def device(target):
        return {"kx": target // ncz, "cz": lax.rem(target, ncz)}

    def held_at(a, kx, part):
        columns = pl.ds(pl.multiple_of(part * local_k, local_k), local_k) if per_share > 1 else slice(None)
        return held.at[pl.ds(a * fields, fields), pl.ds(pl.multiple_of(kx * local_m, local_m), local_m), columns]

    sources = (field_src, adjoint_src)

    def in_remote(a, y):
        return pltpu.make_async_remote_copy(
            src_ref=sources[a].at[y],
            dst_ref=held_at(a, i, my_part),
            send_sem=in_send.at[a, y],
            recv_sem=in_recv.at[a, my_slot],
            device_id=device(y * shares + to_share),
            device_id_type=MESH,
        )

    def in_local(a):
        return pltpu.make_async_copy(sources[a].at[my_y], held_at(a, i, my_part), in_recv.at[a, my_slot])

    for a in range(2):
        @pl.when(stays)
        def _():
            in_local(a).start()

        @pl.when(jnp.logical_not(stays))
        def _():
            in_remote(a, my_y).start()

        def send(step, carry):
            in_remote(a, lax.rem(my_y + step, rows_y)).start()
            return carry

        lax.fori_loop(1, rows_y, send, 0)

    def swap_rows(q):
        return pl.ds(pl.multiple_of(q * share_x, share_x), share_x)

    def swap(a, q):
        arrays = pl.ds(a * fields, fields)
        return pltpu.make_async_remote_copy(
            src_ref=mixed.at[arrays, swap_rows(q), :],
            dst_ref=halves.at[my_share, arrays],
            send_sem=swap_send.at[a, q],
            recv_sem=swap_recv.at[a, my_share],
            device_id=device(my_y * shares + q),
            device_id_type=MESH,
        )

    def swap_local(a):
        arrays = pl.ds(a * fields, fields)
        return pltpu.make_async_copy(
            mixed.at[arrays, swap_rows(my_share), :], halves.at[my_share, arrays], swap_recv.at[a, my_share]
        )

    for a in range(2):
        def arrive(slot, carry):
            pltpu.make_async_copy(
                sources[a].at[0], held_at(a, slot // per_share, lax.rem(slot, per_share)), in_recv.at[a, slot]
            ).wait()
            return carry

        lax.fori_loop(0, rows_y, arrive, 0)

        def mix(f, carry):
            mixed[a * fields + f] = matmul(hartley[...], held[a * fields + f]).astype(jnp.bfloat16)
            return carry

        lax.fori_loop(0, fields, mix, 0)
        swap_local(a).start()
        for step in range(1, shares):
            swap(a, lax.rem(my_share + step, shares)).start()

    for a in range(2):
        for q in range(shares):
            arrays = pl.ds(a * fields, fields)
            pltpu.make_async_copy(
                mixed.at[arrays, swap_rows(0), :], halves.at[q, arrays], swap_recv.at[a, q]
            ).wait()

    tile = 128 if share_x % 128 == 0 else share_x

    def products(step, carry):
        here = pl.ds(pl.multiple_of(step * tile, tile), tile)

        def lifted(a, f):
            table = (lift_fields, lift_adjoint)[a]
            total = matmul(halves[0, a * fields + f, here, :], table[0])
            for q in range(1, shares):
                total += matmul(halves[q, a * fields + f, here, :], table[q])
            return total

        def put(f, value):
            value = value.astype(jnp.bfloat16)
            for q in range(shares):
                lowered[q, f, here, :] = matmul(value, lower[q]).astype(jnp.bfloat16)

        vertical = lifted(0, 2)
        adjoint = lifted(1, 0)
        put(0, adjoint * vertical)
        total = adjoint * lifted(0, 0)
        adjoint = lifted(1, 1)
        put(1, adjoint * vertical)
        total += adjoint * lifted(0, 1)
        total += 2.0 * lifted(1, 2) * vertical
        adjoint = lifted(1, 3)
        put(3, adjoint * vertical)
        total += adjoint * lifted(0, 3)
        put(2, total)
        return carry

    lax.fori_loop(0, share_x // tile, products, 0)

    def back(q):
        return pltpu.make_async_remote_copy(
            src_ref=lowered.at[q],
            dst_ref=turned.at[:, swap_rows(my_share), :],
            send_sem=back_send.at[q],
            recv_sem=back_recv.at[my_share],
            device_id=device(my_y * shares + q),
            device_id_type=MESH,
        )

    back_local = pltpu.make_async_copy(
        lowered.at[my_share], turned.at[:, swap_rows(my_share), :], back_recv.at[my_share]
    )
    back_local.start()
    for step in range(1, shares):
        back(lax.rem(my_share + step, shares)).start()
    for q in range(shares):
        pltpu.make_async_copy(lowered.at[q], turned.at[:, swap_rows(q), :], back_recv.at[q]).wait()

    def result_at(f, slot):
        part = lax.rem(slot, per_share)
        columns = pl.ds(pl.multiple_of(part * local_k, local_k), local_k) if per_share > 1 else slice(None)
        rows = pl.ds(pl.multiple_of((slot // per_share) * local_m, local_m), local_m)
        return result.at[f, rows, columns]

    def owner(slot):
        return (slot // per_share) * ncz + my_share * per_share + lax.rem(slot, per_share)

    def out_remote(f, slot):
        return pltpu.make_async_remote_copy(
            src_ref=result_at(f, slot),
            dst_ref=out.at[my_y, f],
            send_sem=out_send.at[f, slot],
            recv_sem=out_recv.at[f, my_y],
            device_id=device(owner(slot)),
            device_id_type=MESH,
        )

    def out_local(f):
        return pltpu.make_async_copy(result_at(f, my_slot), out.at[my_y, f], out_recv.at[f, my_y])

    def finish(f, carry):
        result[f] = matmul(hartley[...], turned[f]).astype(jnp.bfloat16)

        @pl.when(stays)
        def _():
            out_local(f).start()

        @pl.when(jnp.logical_not(stays))
        def _():
            out_remote(f, my_slot).start()

        def send(step, inner):
            out_remote(f, lax.rem(my_slot + step, rows_y)).start()
            return inner

        lax.fori_loop(1, rows_y, send, 0)
        return carry

    lax.fori_loop(0, fields, finish, 0)

    for a in range(2):
        @pl.when(jnp.logical_not(stays))
        def _():
            in_remote(a, my_y).wait_send()

        def sent(step, carry):
            in_remote(a, lax.rem(my_y + step, rows_y)).wait_send()
            return carry

        lax.fori_loop(1, rows_y, sent, 0)
        for step in range(1, shares):
            swap(a, lax.rem(my_share + step, shares)).wait_send()
    for step in range(1, shares):
        back(lax.rem(my_share + step, shares)).wait_send()

    def close(f, carry):
        @pl.when(jnp.logical_not(stays))
        def _():
            out_remote(f, my_slot).wait_send()

        def sent(step, inner):
            out_remote(f, lax.rem(my_slot + step, rows_y)).wait_send()
            return inner

        lax.fori_loop(1, rows_y, sent, 0)

        def arrive(y, inner):
            pltpu.make_async_copy(result_at(0, 0), out.at[y, f], out_recv.at[f, y]).wait()
            return inner

        lax.fori_loop(0, rows_y, arrive, 0)
        return carry

    lax.fori_loop(0, fields, close, 0)


def on_device(nkx, ncz, field_modes, cotangent):
    local_k, fields, columns = field_modes.shape
    local_m = columns // Y
    modes_z, points_x = local_k * ncz, local_m * nkx
    shares = nkx * ncz // Y
    group_k = modes_z // shares
    share_x = points_x // shares
    bf16 = jnp.bfloat16

    def by_row(array):
        return array.reshape(local_k, fields, local_m, Y).transpose(3, 1, 2, 0)

    cosines = cosine_table(MZ, modes_z)
    synthesis = jnp.asarray((cosines * math.sqrt(2.0 / modes_z)).astype(bf16))
    projection = jnp.asarray((cosines * math.sqrt(2.0 / MZ)).astype(bf16))
    hartley = jnp.asarray(hartley_table(points_x).astype(np.float32).astype(bf16))
    lift_fields = synthesis.T.reshape(shares, group_k, MZ)
    lift_adjoint = projection.T.reshape(shares, group_k, MZ)
    lower = synthesis.reshape(MZ, shares, group_k).transpose(1, 0, 2)

    vmem = pl.BlockSpec(memory_space=pltpu.VMEM)
    dma = pltpu.SemaphoreType.DMA
    out = pl.pallas_call(
        functools.partial(kernel, nkx, ncz, shares),
        out_shape=jax.ShapeDtypeStruct((Y, fields, local_m, local_k), bf16),
        in_specs=[vmem] * 6,
        out_specs=pl.BlockSpec(memory_space=pl.ANY),
        scratch_shapes=[
            pltpu.VMEM((2 * fields, points_x, group_k), bf16),
            pltpu.VMEM((2 * fields, points_x, group_k), bf16),
            pltpu.VMEM((shares, 2 * fields, share_x, group_k), bf16),
            pltpu.VMEM((shares, fields, share_x, group_k), bf16),
            pltpu.VMEM((fields, points_x, group_k), bf16),
            pltpu.VMEM((fields, points_x, group_k), bf16),
            dma((2, Y)), dma((2, Y)), dma((2, shares)), dma((2, shares)),
            dma((shares,)), dma((shares,)), dma((fields, Y)), dma((fields, Y)),
        ],
        compiler_params=pltpu.CompilerParams(has_side_effects=True, vmem_limit_bytes=48 * 2**20),
    )(by_row(field_modes), by_row(cotangent), hartley, lift_fields, lift_adjoint, lower)
    return out.transpose(3, 1, 2, 0).reshape(local_k, fields, columns)


def solution(mesh):
    return jax.shard_map(
        functools.partial(on_device, mesh.shape["kx"], mesh.shape["cz"]),
        mesh=mesh,
        in_specs=(P("cz", None, "kx"), P("cz", None, "kx")),
        out_specs=P("cz", None, "kx"),
        check_vma=False,
    )
```

```python
import functools
import math

import jax
import jax.numpy as jnp
import numpy as np
from jax import lax
from jax.experimental import pallas as pl
from jax.experimental.pallas import tpu as pltpu
from jax.sharding import PartitionSpec as P

MZ = 768
Y = 16
MESH = pl.DeviceIdType.MESH


def cosine_table(rows, columns):
    position = (np.arange(columns)[None, :] * (2 * np.arange(rows)[:, None] + 1)) % (4 * rows)
    return np.cos(np.pi * position / (2 * rows)).astype(np.float32)


def hartley_table(points):
    index = np.arange(points)
    phases = 2.0 * np.pi * ((index[:, None] * index[None, :]) % points) / points
    return (np.cos(phases) + np.sin(phases)) / math.sqrt(points)


def matmul(a, b):
    return jnp.dot(a, b, preferred_element_type=jnp.float32)


def kernel(
    nkx, ncz, shares,
    field_src, adjoint_src, hartley, lift_fields, lift_adjoint, lower,
    out,
    held, mixed, halves, points, total, flux, lowered, turned, result,
    in_send, in_recv, swap_send, swap_recv, back_send, back_recv, out_send, out_recv,
):
    rows_y, fields, local_m, local_k = field_src.shape
    per_share = ncz // shares
    points_x = hartley.shape[0]
    points_z = lift_fields.shape[2]
    share_x = points_x // shares
    i, j = lax.axis_index("kx"), lax.axis_index("cz")
    linear = i * ncz + j
    my_y, my_share = linear // shares, lax.rem(linear, shares)
    to_share = j // per_share
    my_part = lax.rem(j, per_share)
    my_slot = i * per_share + my_part
    stays = to_share == my_share
    far = rows_y // 2
    order = ((0, 2), (1, 0), (1, 1), (1, 3), (0, 0), (0, 1), (0, 3), (1, 2))
    sources = (field_src, adjoint_src)
    tables = (lift_fields, lift_adjoint)

    def device(target):
        return {"kx": target // ncz, "cz": lax.rem(target, ncz)}

    def block(ref, slot):
        part = lax.rem(slot, per_share)
        rows = pl.ds(pl.multiple_of((slot // per_share) * local_m, local_m), local_m)
        columns = pl.ds(pl.multiple_of(part * local_k, local_k), local_k) if per_share > 1 else slice(None)
        return ref.at[rows, columns]

    def other(mine, step):
        half = jnp.where(step < far, 1 - mine // far, mine // far)
        return half * far + lax.rem(mine + 1 + step, far)

    def wait(ref, sem):
        pltpu.make_async_copy(ref, ref, sem).wait()

    def in_remote(h, y):
        a, f = order[h]
        return pltpu.make_async_remote_copy(
            src_ref=sources[a].at[y, f],
            dst_ref=block(held.at[h], my_slot),
            send_sem=in_send.at[a],
            recv_sem=in_recv.at[h],
            device_id=device(y * shares + to_share),
            device_id_type=MESH,
        )

    for h, (a, f) in enumerate(order):
        def send(step, carry):
            in_remote(h, other(my_y, step)).start()
            return carry

        lax.fori_loop(0, rows_y - 1, send, 0)

        @pl.when(stays)
        def _():
            pltpu.make_async_copy(sources[a].at[my_y, f], block(held.at[h], my_slot), in_recv.at[h]).start()

        @pl.when(jnp.logical_not(stays))
        def _():
            in_remote(h, my_y).start()

    def share_rows(q):
        return pl.ds(pl.multiple_of(q * share_x, share_x), share_x)

    def mix(h):
        wait(held.at[h], in_recv.at[h])
        mixed[h] = matmul(hartley[...], held[h]).astype(jnp.bfloat16)
        for step in range(1, shares):
            q = lax.rem(my_share + step, shares)
            pltpu.make_async_remote_copy(
                src_ref=mixed.at[h, share_rows(q), :],
                dst_ref=halves.at[h, my_share],
                send_sem=swap_send,
                recv_sem=swap_recv.at[h],
                device_id=device(my_y * shares + q),
                device_id_type=MESH,
            ).start()
        pltpu.make_async_copy(
            mixed.at[h, share_rows(my_share), :], halves.at[h, my_share], swap_recv.at[h]
        ).start()

    block_z = 256 if points_z % 256 == 0 else points_z

    def lift(h, use):
        wait(halves.at[h], swap_recv.at[h])
        table = tables[order[h][0]]

        def one(step, carry):
            here = pl.ds(pl.multiple_of(step * block_z, block_z), block_z)
            value = matmul(halves[h, 0], table[0, :, here])
            for q in range(1, shares):
                value += matmul(halves[h, q], table[q, :, here])
            use(here, value)
            return carry

        lax.fori_loop(0, points_z // block_z, one, 0)

    def leave(f):
        for q in range(shares):
            lowered[f, q] = matmul(flux[...], lower[q]).astype(jnp.bfloat16)
        for step in range(1, shares):
            q = lax.rem(my_share + step, shares)
            pltpu.make_async_remote_copy(
                src_ref=lowered.at[f, q],
                dst_ref=turned.at[f, share_rows(my_share), :],
                send_sem=back_send,
                recv_sem=back_recv.at[f],
                device_id=device(my_y * shares + q),
                device_id_type=MESH,
            ).start()
        pltpu.make_async_copy(
            lowered.at[f, my_share], turned.at[f, share_rows(my_share), :], back_recv.at[f]
        ).start()

    def out_remote(f, slot):
        target = (slot // per_share) * ncz + my_share * per_share + lax.rem(slot, per_share)
        return pltpu.make_async_remote_copy(
            src_ref=block(result.at[f], slot),
            dst_ref=out.at[my_y, f],
            send_sem=out_send,
            recv_sem=out_recv.at[f],
            device_id=device(target),
            device_id_type=MESH,
        )

    def finish(f):
        wait(turned.at[f], back_recv.at[f])
        result[f] = matmul(hartley[...], turned[f]).astype(jnp.bfloat16)

        def send(step, carry):
            out_remote(f, other(my_slot, step)).start()
            return carry

        lax.fori_loop(0, rows_y - 1, send, 0)

        @pl.when(stays)
        def _():
            pltpu.make_async_copy(block(result.at[f], my_slot), out.at[my_y, f], out_recv.at[f]).start()

        @pl.when(jnp.logical_not(stays))
        def _():
            out_remote(f, my_slot).start()

    def keep(h):
        def use(here, value):
            points[h, :, here] = value
        return use

    def keep_and_flux(h):
        def use(here, value):
            points[h, :, here] = value
            flux[:, here] = (value * points[0, :, here]).astype(jnp.bfloat16)
        return use

    def first(here, value):
        total[:, here] = points[1, :, here] * value

    def add(h):
        def use(here, value):
            total[:, here] += points[h, :, here] * value
        return use

    def last(here, value):
        flux[:, here] = (total[:, here] + 2.0 * value * points[0, :, here]).astype(jnp.bfloat16)

    mix(0)
    mix(1)
    lift(0, keep(0))
    lift(1, keep_and_flux(1))
    leave(0)
    mix(2)
    finish(0)
    lift(2, keep_and_flux(2))
    leave(1)
    mix(3)
    finish(1)
    lift(3, keep_and_flux(3))
    leave(3)
    mix(4)
    finish(3)
    lift(4, first)
    mix(5)
    lift(5, add(2))
    mix(6)
    lift(6, add(3))
    mix(7)
    lift(7, last)
    leave(2)
    finish(2)

    for a in range(2):
        @pl.when(stays)
        def _():
            wait(sources[a].at[pl.ds(0, rows_y - 1)], in_send.at[a])

        @pl.when(jnp.logical_not(stays))
        def _():
            wait(sources[a], in_send.at[a])

    if shares > 1:
        wait(mixed.at[:, pl.ds(0, share_x * (shares - 1)), :], swap_send)
        wait(lowered.at[:, pl.ds(0, shares - 1)], back_send)

    @pl.when(stays)
    def _():
        wait(out.at[pl.ds(0, rows_y - 1)], out_send)

    @pl.when(jnp.logical_not(stays))
    def _():
        wait(out, out_send)

    for f in range(fields):
        wait(out.at[:, f], out_recv.at[f])


def on_device(nkx, ncz, field_modes, cotangent):
    local_k, fields, columns = field_modes.shape
    local_m = columns // Y
    modes_z, points_x = local_k * ncz, local_m * nkx
    shares = nkx * ncz // Y
    group_k = modes_z // shares
    share_x = points_x // shares
    bf16 = jnp.bfloat16

    def by_row(array):
        return array.reshape(local_k, fields, local_m, Y).transpose(3, 1, 2, 0)

    cosines = cosine_table(MZ, modes_z)
    synthesis = jnp.asarray((cosines * math.sqrt(2.0 / modes_z)).astype(bf16))
    projection = jnp.asarray((cosines * math.sqrt(2.0 / MZ)).astype(bf16))
    hartley = jnp.asarray(hartley_table(points_x).astype(np.float32).astype(bf16))
    lift_fields = synthesis.T.reshape(shares, group_k, MZ)
    lift_adjoint = projection.T.reshape(shares, group_k, MZ)
    lower = synthesis.reshape(MZ, shares, group_k).transpose(1, 0, 2)

    vmem = pl.BlockSpec(memory_space=pltpu.VMEM)
    dma = pltpu.SemaphoreType.DMA
    out = pl.pallas_call(
        functools.partial(kernel, nkx, ncz, shares),
        out_shape=jax.ShapeDtypeStruct((Y, fields, local_m, local_k), bf16),
        in_specs=[vmem] * 6,
        out_specs=pl.BlockSpec(memory_space=pl.ANY),
        scratch_shapes=[
            pltpu.VMEM((2 * fields, points_x, group_k), bf16),
            pltpu.VMEM((2 * fields, points_x, group_k), bf16),
            pltpu.VMEM((2 * fields, shares, share_x, group_k), bf16),
            pltpu.VMEM((fields, share_x, MZ), jnp.float32),
            pltpu.VMEM((share_x, MZ), jnp.float32),
            pltpu.VMEM((share_x, MZ), bf16),
            pltpu.VMEM((fields, shares, share_x, group_k), bf16),
            pltpu.VMEM((fields, points_x, group_k), bf16),
            pltpu.VMEM((fields, points_x, group_k), bf16),
            dma((2,)), dma((2 * fields,)), dma, dma((2 * fields,)),
            dma, dma((fields,)), dma, dma((fields,)),
        ],
        compiler_params=pltpu.CompilerParams(has_side_effects=True, vmem_limit_bytes=48 * 2**20),
    )(by_row(field_modes), by_row(cotangent), hartley, lift_fields, lift_adjoint, lower)
    return out.transpose(3, 1, 2, 0).reshape(local_k, fields, columns)


def solution(mesh):
    return jax.shard_map(
        functools.partial(on_device, mesh.shape["kx"], mesh.shape["cz"]),
        mesh=mesh,
        in_specs=(P("cz", None, "kx"), P("cz", None, "kx")),
        out_specs=P("cz", None, "kx"),
        check_vma=False,
    )
```

```python
import functools
import math

import jax
import jax.numpy as jnp
import numpy as np
from jax import lax
from jax.experimental import pallas as pl
from jax.experimental.pallas import tpu as pltpu
from jax.sharding import PartitionSpec as P

MZ = 768
Y = 16
MESH = pl.DeviceIdType.MESH


def cosine_table(rows, columns):
    position = (np.arange(columns)[None, :] * (2 * np.arange(rows)[:, None] + 1)) % (4 * rows)
    return np.cos(np.pi * position / (2 * rows)).astype(np.float32)


def hartley_table(points):
    index = np.arange(points)
    phases = 2.0 * np.pi * ((index[:, None] * index[None, :]) % points) / points
    return (np.cos(phases) + np.sin(phases)) / math.sqrt(points)


def matmul(a, b):
    return jnp.dot(a, b, preferred_element_type=jnp.float32)


def kernel(
    nkx, ncz, shares,
    field_modes, cotangent, hartley, lift_fields, lift_adjoint, lower,
    out,
    wide, rows, held, mixed, halves, points, total, flux, lowered, turned, result,
    in_send, in_recv, swap_send, swap_recv, back_send, back_recv, out_send, out_recv,
):
    local_k, fields, columns = field_modes.shape
    rows_y = rows.shape[1]
    local_m = columns // rows_y
    per_share = ncz // shares
    points_x = hartley.shape[0]
    points_z = lift_fields.shape[2]
    share_x = points_x // shares
    i, j = lax.axis_index("kx"), lax.axis_index("cz")
    linear = i * ncz + j
    my_y, my_share = linear // shares, lax.rem(linear, shares)
    to_share = j // per_share
    my_part = lax.rem(j, per_share)
    my_slot = i * per_share + my_part
    stays = to_share == my_share
    far = rows_y // 2
    order = ((0, 2), (1, 0), (1, 1), (1, 3), (0, 0), (0, 1), (0, 3), (1, 2))
    sources = (field_modes, cotangent)
    tables = (lift_fields, lift_adjoint)

    def device(target):
        return {"kx": target // ncz, "cz": lax.rem(target, ncz)}

    def block(ref, slot):
        part = lax.rem(slot, per_share)
        rows = pl.ds(pl.multiple_of((slot // per_share) * local_m, local_m), local_m)
        columns = pl.ds(pl.multiple_of(part * local_k, local_k), local_k) if per_share > 1 else slice(None)
        return ref.at[rows, columns]

    def other(mine, step):
        half = jnp.where(step < far, 1 - mine // far, mine // far)
        return half * far + lax.rem(mine + 1 + step, far)

    def wait(ref, sem):
        pltpu.make_async_copy(ref, ref, sem).wait()

    def in_remote(h, y):
        return pltpu.make_async_remote_copy(
            src_ref=rows.at[h, y],
            dst_ref=block(held.at[h], my_slot),
            send_sem=in_send,
            recv_sem=in_recv.at[h],
            device_id=device(y * shares + to_share),
            device_id_type=MESH,
        )

    chunk = 128 if columns % 128 == 0 else columns

    for h, (a, f) in enumerate(order):
        def turn(step, carry):
            here = pl.ds(pl.multiple_of(step * chunk, chunk), chunk)
            wide[here, :] = sources[a][:, f, here].astype(jnp.float32).T
            return carry

        lax.fori_loop(0, columns // chunk, turn, 0)
        for y in range(rows_y):
            rows[h, y] = wide[pl.ds(y, local_m, stride=rows_y), :].astype(jnp.bfloat16)

        def send(step, carry):
            in_remote(h, other(my_y, step)).start()
            return carry

        lax.fori_loop(0, rows_y - 1, send, 0)

        @pl.when(stays)
        def _():
            pltpu.make_async_copy(rows.at[h, my_y], block(held.at[h], my_slot), in_recv.at[h]).start()

        @pl.when(jnp.logical_not(stays))
        def _():
            in_remote(h, my_y).start()

    def share_rows(q):
        return pl.ds(pl.multiple_of(q * share_x, share_x), share_x)

    def mix(h):
        wait(held.at[h], in_recv.at[h])
        mixed[h] = matmul(hartley[...], held[h]).astype(jnp.bfloat16)
        for step in range(1, shares):
            q = lax.rem(my_share + step, shares)
            pltpu.make_async_remote_copy(
                src_ref=mixed.at[h, share_rows(q), :],
                dst_ref=halves.at[h, my_share],
                send_sem=swap_send,
                recv_sem=swap_recv.at[h],
                device_id=device(my_y * shares + q),
                device_id_type=MESH,
            ).start()
        pltpu.make_async_copy(
            mixed.at[h, share_rows(my_share), :], halves.at[h, my_share], swap_recv.at[h]
        ).start()

    block_z = 256 if points_z % 256 == 0 else points_z

    def lift(h, use):
        wait(halves.at[h], swap_recv.at[h])
        table = tables[order[h][0]]

        def one(step, carry):
            here = pl.ds(pl.multiple_of(step * block_z, block_z), block_z)
            value = matmul(halves[h, 0], table[0, :, here])
            for q in range(1, shares):
                value += matmul(halves[h, q], table[q, :, here])
            use(here, value)
            return carry

        lax.fori_loop(0, points_z // block_z, one, 0)

    def leave(f):
        for q in range(shares):
            lowered[f, q] = matmul(flux[...], lower[q]).astype(jnp.bfloat16)
        for step in range(1, shares):
            q = lax.rem(my_share + step, shares)
            pltpu.make_async_remote_copy(
                src_ref=lowered.at[f, q],
                dst_ref=turned.at[f, share_rows(my_share), :],
                send_sem=back_send,
                recv_sem=back_recv.at[f],
                device_id=device(my_y * shares + q),
                device_id_type=MESH,
            ).start()
        pltpu.make_async_copy(
            lowered.at[f, my_share], turned.at[f, share_rows(my_share), :], back_recv.at[f]
        ).start()

    def out_remote(f, slot):
        target = (slot // per_share) * ncz + my_share * per_share + lax.rem(slot, per_share)
        return pltpu.make_async_remote_copy(
            src_ref=block(result.at[f], slot),
            dst_ref=out.at[my_y, f],
            send_sem=out_send,
            recv_sem=out_recv.at[f],
            device_id=device(target),
            device_id_type=MESH,
        )

    def finish(f):
        wait(turned.at[f], back_recv.at[f])
        result[f] = matmul(hartley[...], turned[f]).astype(jnp.bfloat16)

        def send(step, carry):
            out_remote(f, other(my_slot, step)).start()
            return carry

        lax.fori_loop(0, rows_y - 1, send, 0)

        @pl.when(stays)
        def _():
            pltpu.make_async_copy(block(result.at[f], my_slot), out.at[my_y, f], out_recv.at[f]).start()

        @pl.when(jnp.logical_not(stays))
        def _():
            out_remote(f, my_slot).start()

    def keep(h):
        def use(here, value):
            points[h, :, here] = value
        return use

    def keep_and_flux(h):
        def use(here, value):
            points[h, :, here] = value
            flux[:, here] = (value * points[0, :, here]).astype(jnp.bfloat16)
        return use

    def first(here, value):
        total[:, here] = points[1, :, here] * value

    def add(h):
        def use(here, value):
            total[:, here] += points[h, :, here] * value
        return use

    def last(here, value):
        flux[:, here] = (total[:, here] + 2.0 * value * points[0, :, here]).astype(jnp.bfloat16)

    mix(0)
    mix(1)
    lift(0, keep(0))
    lift(1, keep_and_flux(1))
    leave(0)
    mix(2)
    finish(0)
    lift(2, keep_and_flux(2))
    leave(1)
    mix(3)
    finish(1)
    lift(3, keep_and_flux(3))
    leave(3)
    mix(4)
    finish(3)
    lift(4, first)
    mix(5)
    lift(5, add(2))
    mix(6)
    lift(6, add(3))
    mix(7)
    lift(7, last)
    leave(2)
    finish(2)

    @pl.when(stays)
    def _():
        wait(rows.at[:, pl.ds(0, rows_y - 1)], in_send)

    @pl.when(jnp.logical_not(stays))
    def _():
        wait(rows, in_send)

    if shares > 1:
        wait(mixed.at[:, pl.ds(0, share_x * (shares - 1)), :], swap_send)
        wait(lowered.at[:, pl.ds(0, shares - 1)], back_send)

    @pl.when(stays)
    def _():
        wait(out.at[pl.ds(0, rows_y - 1)], out_send)

    @pl.when(jnp.logical_not(stays))
    def _():
        wait(out, out_send)

    for f in range(fields):
        wait(out.at[:, f], out_recv.at[f])


def on_device(nkx, ncz, field_modes, cotangent):
    local_k, fields, columns = field_modes.shape
    local_m = columns // Y
    modes_z, points_x = local_k * ncz, local_m * nkx
    shares = nkx * ncz // Y
    group_k = modes_z // shares
    share_x = points_x // shares
    bf16 = jnp.bfloat16

    cosines = cosine_table(MZ, modes_z)
    synthesis = jnp.asarray((cosines * math.sqrt(2.0 / modes_z)).astype(bf16))
    projection = jnp.asarray((cosines * math.sqrt(2.0 / MZ)).astype(bf16))
    hartley = jnp.asarray(hartley_table(points_x).astype(np.float32).astype(bf16))
    lift_fields = synthesis.T.reshape(shares, group_k, MZ)
    lift_adjoint = projection.T.reshape(shares, group_k, MZ)
    lower = synthesis.reshape(MZ, shares, group_k).transpose(1, 0, 2)

    vmem = pl.BlockSpec(memory_space=pltpu.VMEM)
    dma = pltpu.SemaphoreType.DMA
    out = pl.pallas_call(
        functools.partial(kernel, nkx, ncz, shares),
        out_shape=jax.ShapeDtypeStruct((Y, fields, local_m, local_k), bf16),
        in_specs=[vmem] * 6,
        out_specs=pl.BlockSpec(memory_space=pl.ANY),
        scratch_shapes=[
            pltpu.VMEM((columns, local_k), jnp.float32),
            pltpu.VMEM((2 * fields, Y, local_m, local_k), bf16),
            pltpu.VMEM((2 * fields, points_x, group_k), bf16),
            pltpu.VMEM((2 * fields, points_x, group_k), bf16),
            pltpu.VMEM((2 * fields, shares, share_x, group_k), bf16),
            pltpu.VMEM((fields, share_x, MZ), jnp.float32),
            pltpu.VMEM((share_x, MZ), jnp.float32),
            pltpu.VMEM((share_x, MZ), bf16),
            pltpu.VMEM((fields, shares, share_x, group_k), bf16),
            pltpu.VMEM((fields, points_x, group_k), bf16),
            pltpu.VMEM((fields, points_x, group_k), bf16),
            dma, dma((2 * fields,)), dma, dma((2 * fields,)),
            dma, dma((fields,)), dma, dma((fields,)),
        ],
        compiler_params=pltpu.CompilerParams(has_side_effects=True, vmem_limit_bytes=48 * 2**20),
    )(field_modes, cotangent, hartley, lift_fields, lift_adjoint, lower)
    return out.transpose(3, 1, 2, 0).reshape(local_k, fields, columns)


def solution(mesh):
    return jax.shard_map(
        functools.partial(on_device, mesh.shape["kx"], mesh.shape["cz"]),
        mesh=mesh,
        in_specs=(P("cz", None, "kx"), P("cz", None, "kx")),
        out_specs=P("cz", None, "kx"),
        check_vma=False,
    )
```

```python
import functools
import math

import jax
import jax.numpy as jnp
import numpy as np
from jax import lax
from jax.experimental import pallas as pl
from jax.experimental.pallas import tpu as pltpu
from jax.sharding import PartitionSpec as P

MZ = 768
Y = 16
MESH = pl.DeviceIdType.MESH


def cosine_table(rows, columns):
    position = (np.arange(columns)[None, :] * (2 * np.arange(rows)[:, None] + 1)) % (4 * rows)
    return np.cos(np.pi * position / (2 * rows)).astype(np.float32)


def hartley_table(points):
    index = np.arange(points)
    phases = 2.0 * np.pi * ((index[:, None] * index[None, :]) % points) / points
    return (np.cos(phases) + np.sin(phases)) / math.sqrt(points)


def matmul(a, b):
    return jnp.dot(a, b, preferred_element_type=jnp.float32)


def kernel(
    nkx, ncz, shares,
    field_modes, cotangent, hartley_in, lift_fields_in, lift_adjoint_in, lower_in,
    out,
    raw, hartley, lift_fields, lift_adjoint, lower, raw_sem, table_sem,
    wide, rows, held, mixed, halves, points, total, flux, lowered, turned, result,
    in_send, in_recv, swap_send, swap_recv, back_send, back_recv, out_send, out_recv,
):
    local_k, fields, columns = field_modes.shape
    rows_y = rows.shape[1]
    local_m = columns // rows_y
    per_share = ncz // shares
    points_x = hartley.shape[0]
    points_z = lift_fields.shape[2]
    share_x = points_x // shares
    i, j = lax.axis_index("kx"), lax.axis_index("cz")
    linear = i * ncz + j
    my_y, my_share = linear // shares, lax.rem(linear, shares)
    to_share = j // per_share
    my_part = lax.rem(j, per_share)
    my_slot = i * per_share + my_part
    stays = to_share == my_share
    far = rows_y // 2
    order = ((0, 2), (1, 0), (1, 1), (1, 3), (0, 0), (0, 1), (0, 3), (1, 2))
    raw_copies = [
        pltpu.make_async_copy(array, raw.at[a], raw_sem.at[a]) for a, array in enumerate((field_modes, cotangent))
    ]
    table_copies = [
        pltpu.make_async_copy(source, target, table_sem.at[n])
        for n, (source, target) in enumerate(
            (
                (hartley_in, hartley),
                (lift_fields_in, lift_fields),
                (lift_adjoint_in, lift_adjoint),
                (lower_in, lower),
            )
        )
    ]
    for copy in raw_copies + table_copies:
        copy.start()
    tables = (lift_fields, lift_adjoint)

    def device(target):
        return {"kx": target // ncz, "cz": lax.rem(target, ncz)}

    def block(ref, slot):
        part = lax.rem(slot, per_share)
        rows = pl.ds(pl.multiple_of((slot // per_share) * local_m, local_m), local_m)
        columns = pl.ds(pl.multiple_of(part * local_k, local_k), local_k) if per_share > 1 else slice(None)
        return ref.at[rows, columns]

    def other(mine, step):
        half = jnp.where(step < far, 1 - mine // far, mine // far)
        return half * far + lax.rem(mine + 1 + step, far)

    def wait(ref, sem):
        pltpu.make_async_copy(ref, ref, sem).wait()

    def in_remote(h, y):
        return pltpu.make_async_remote_copy(
            src_ref=rows.at[h, y],
            dst_ref=block(held.at[h], my_slot),
            send_sem=in_send,
            recv_sem=in_recv.at[h],
            device_id=device(y * shares + to_share),
            device_id_type=MESH,
        )

    chunk = 128 if columns % 128 == 0 else columns

    for h, (a, f) in enumerate(order):
        if h < 2:
            raw_copies[h].wait()

        def turn(step, carry):
            here = pl.ds(pl.multiple_of(step * chunk, chunk), chunk)
            wide[here, :] = raw[a, :, f, here].astype(jnp.float32).T
            return carry

        lax.fori_loop(0, columns // chunk, turn, 0)
        for y in range(rows_y):
            rows[h, y] = wide[pl.ds(y, local_m, stride=rows_y), :].astype(jnp.bfloat16)

        def send(step, carry):
            in_remote(h, other(my_y, step)).start()
            return carry

        lax.fori_loop(0, rows_y - 1, send, 0)

        @pl.when(stays)
        def _():
            pltpu.make_async_copy(rows.at[h, my_y], block(held.at[h], my_slot), in_recv.at[h]).start()

        @pl.when(jnp.logical_not(stays))
        def _():
            in_remote(h, my_y).start()

    def share_rows(q):
        return pl.ds(pl.multiple_of(q * share_x, share_x), share_x)

    def mix(h):
        wait(held.at[h], in_recv.at[h])
        mixed[h] = matmul(hartley[...], held[h]).astype(jnp.bfloat16)
        for step in range(1, shares):
            q = lax.rem(my_share + step, shares)
            pltpu.make_async_remote_copy(
                src_ref=mixed.at[h, share_rows(q), :],
                dst_ref=halves.at[h, my_share],
                send_sem=swap_send,
                recv_sem=swap_recv.at[h],
                device_id=device(my_y * shares + q),
                device_id_type=MESH,
            ).start()
        pltpu.make_async_copy(
            mixed.at[h, share_rows(my_share), :], halves.at[h, my_share], swap_recv.at[h]
        ).start()

    block_z = 256 if points_z % 256 == 0 else points_z

    def lift(h, use):
        wait(halves.at[h], swap_recv.at[h])
        table = tables[order[h][0]]

        def one(step, carry):
            here = pl.ds(pl.multiple_of(step * block_z, block_z), block_z)
            value = matmul(halves[h, 0], table[0, :, here])
            for q in range(1, shares):
                value += matmul(halves[h, q], table[q, :, here])
            use(here, value)
            return carry

        lax.fori_loop(0, points_z // block_z, one, 0)

    def leave(f):
        for q in range(shares):
            lowered[f, q] = matmul(flux[...], lower[q]).astype(jnp.bfloat16)
        for step in range(1, shares):
            q = lax.rem(my_share + step, shares)
            pltpu.make_async_remote_copy(
                src_ref=lowered.at[f, q],
                dst_ref=turned.at[f, share_rows(my_share), :],
                send_sem=back_send,
                recv_sem=back_recv.at[f],
                device_id=device(my_y * shares + q),
                device_id_type=MESH,
            ).start()
        pltpu.make_async_copy(
            lowered.at[f, my_share], turned.at[f, share_rows(my_share), :], back_recv.at[f]
        ).start()

    def out_remote(f, slot):
        target = (slot // per_share) * ncz + my_share * per_share + lax.rem(slot, per_share)
        return pltpu.make_async_remote_copy(
            src_ref=block(result.at[f], slot),
            dst_ref=out.at[my_y, f],
            send_sem=out_send,
            recv_sem=out_recv.at[f],
            device_id=device(target),
            device_id_type=MESH,
        )

    def finish(f):
        wait(turned.at[f], back_recv.at[f])
        result[f] = matmul(hartley[...], turned[f]).astype(jnp.bfloat16)

        def send(step, carry):
            out_remote(f, other(my_slot, step)).start()
            return carry

        lax.fori_loop(0, rows_y - 1, send, 0)

        @pl.when(stays)
        def _():
            pltpu.make_async_copy(block(result.at[f], my_slot), out.at[my_y, f], out_recv.at[f]).start()

        @pl.when(jnp.logical_not(stays))
        def _():
            out_remote(f, my_slot).start()

    def keep(h):
        def use(here, value):
            points[h, :, here] = value
        return use

    def keep_and_flux(h):
        def use(here, value):
            points[h, :, here] = value
            flux[:, here] = (value * points[0, :, here]).astype(jnp.bfloat16)
        return use

    def first(here, value):
        total[:, here] = points[1, :, here] * value

    def add(h):
        def use(here, value):
            total[:, here] += points[h, :, here] * value
        return use

    def last(here, value):
        flux[:, here] = (total[:, here] + 2.0 * value * points[0, :, here]).astype(jnp.bfloat16)

    for copy in table_copies:
        copy.wait()
    mix(0)
    mix(1)
    lift(0, keep(0))
    lift(1, keep_and_flux(1))
    leave(0)
    mix(2)
    finish(0)
    lift(2, keep_and_flux(2))
    leave(1)
    mix(3)
    finish(1)
    lift(3, keep_and_flux(3))
    leave(3)
    mix(4)
    finish(3)
    lift(4, first)
    mix(5)
    lift(5, add(2))
    mix(6)
    lift(6, add(3))
    mix(7)
    lift(7, last)
    leave(2)
    finish(2)

    @pl.when(stays)
    def _():
        wait(rows.at[:, pl.ds(0, rows_y - 1)], in_send)

    @pl.when(jnp.logical_not(stays))
    def _():
        wait(rows, in_send)

    if shares > 1:
        wait(mixed.at[:, pl.ds(0, share_x * (shares - 1)), :], swap_send)
        wait(lowered.at[:, pl.ds(0, shares - 1)], back_send)

    @pl.when(stays)
    def _():
        wait(out.at[pl.ds(0, rows_y - 1)], out_send)

    @pl.when(jnp.logical_not(stays))
    def _():
        wait(out, out_send)

    for f in range(fields):
        wait(out.at[:, f], out_recv.at[f])


def on_device(nkx, ncz, field_modes, cotangent):
    local_k, fields, columns = field_modes.shape
    local_m = columns // Y
    modes_z, points_x = local_k * ncz, local_m * nkx
    shares = nkx * ncz // Y
    group_k = modes_z // shares
    share_x = points_x // shares
    bf16 = jnp.bfloat16

    cosines = cosine_table(MZ, modes_z)
    synthesis = jnp.asarray((cosines * math.sqrt(2.0 / modes_z)).astype(bf16))
    projection = jnp.asarray((cosines * math.sqrt(2.0 / MZ)).astype(bf16))
    hartley = jnp.asarray(hartley_table(points_x).astype(np.float32).astype(bf16))
    lift_fields = synthesis.T.reshape(shares, group_k, MZ)
    lift_adjoint = projection.T.reshape(shares, group_k, MZ)
    lower = synthesis.reshape(MZ, shares, group_k).transpose(1, 0, 2)

    hbm = pl.BlockSpec(memory_space=pltpu.HBM)
    dma = pltpu.SemaphoreType.DMA
    out = pl.pallas_call(
        functools.partial(kernel, nkx, ncz, shares),
        out_shape=jax.ShapeDtypeStruct((Y, fields, local_m, local_k), bf16),
        in_specs=[hbm] * 6,
        out_specs=pl.BlockSpec(memory_space=pl.ANY),
        scratch_shapes=[
            pltpu.VMEM((2, local_k, fields, columns), bf16),
            pltpu.VMEM(hartley.shape, bf16),
            pltpu.VMEM(lift_fields.shape, bf16),
            pltpu.VMEM(lift_adjoint.shape, bf16),
            pltpu.VMEM(lower.shape, bf16),
            dma((2,)), dma((4,)),
            pltpu.VMEM((columns, local_k), jnp.float32),
            pltpu.VMEM((2 * fields, Y, local_m, local_k), bf16),
            pltpu.VMEM((2 * fields, points_x, group_k), bf16),
            pltpu.VMEM((2 * fields, points_x, group_k), bf16),
            pltpu.VMEM((2 * fields, shares, share_x, group_k), bf16),
            pltpu.VMEM((fields, share_x, MZ), jnp.float32),
            pltpu.VMEM((share_x, MZ), jnp.float32),
            pltpu.VMEM((share_x, MZ), bf16),
            pltpu.VMEM((fields, shares, share_x, group_k), bf16),
            pltpu.VMEM((fields, points_x, group_k), bf16),
            pltpu.VMEM((fields, points_x, group_k), bf16),
            dma, dma((2 * fields,)), dma, dma((2 * fields,)),
            dma, dma((fields,)), dma, dma((fields,)),
        ],
        compiler_params=pltpu.CompilerParams(has_side_effects=True, vmem_limit_bytes=48 * 2**20),
    )(field_modes, cotangent, hartley, lift_fields, lift_adjoint, lower)
    return out.transpose(3, 1, 2, 0).reshape(local_k, fields, columns)


def solution(mesh):
    return jax.shard_map(
        functools.partial(on_device, mesh.shape["kx"], mesh.shape["cz"]),
        mesh=mesh,
        in_specs=(P("cz", None, "kx"), P("cz", None, "kx")),
        out_specs=P("cz", None, "kx"),
        check_vma=False,
    )
```

```python
import functools
import math

import jax
import jax.numpy as jnp
import numpy as np
from jax import lax
from jax.experimental import pallas as pl
from jax.experimental.pallas import tpu as pltpu
from jax.sharding import PartitionSpec as P

MZ = 768
Y = 16
MESH = pl.DeviceIdType.MESH


def cosine_table(rows, columns):
    position = (np.arange(columns)[None, :] * (2 * np.arange(rows)[:, None] + 1)) % (4 * rows)
    return np.cos(np.pi * position / (2 * rows)).astype(np.float32)


def hartley_table(points):
    index = np.arange(points)
    phases = 2.0 * np.pi * ((index[:, None] * index[None, :]) % points) / points
    return (np.cos(phases) + np.sin(phases)) / math.sqrt(points)


def matmul(a, b):
    return jnp.dot(a, b, preferred_element_type=jnp.float32)


def kernel(
    nkx, ncz, shares,
    field_modes, cotangent, hartley_in, lift_fields_in, lift_adjoint_in, lower_in,
    out,
    raw, hartley, lift_fields, lift_adjoint, lower, raw_sem, table_sem,
    wide, rows, landed, held, mixed, halves, points, total, flux, lowered, turned, result,
    in_send, in_recv, swap_send, swap_recv, back_send, back_recv, out_send, out_recv,
):
    local_k, fields, columns = field_modes.shape
    rows_y = rows.shape[1]
    local_m = columns // rows_y
    per_share = ncz // shares
    points_x = hartley.shape[0]
    points_z = lift_fields.shape[2]
    share_x = points_x // shares
    i, j = lax.axis_index("kx"), lax.axis_index("cz")
    linear = i * ncz + j
    my_y, my_share = linear // shares, lax.rem(linear, shares)
    to_share = j // per_share
    my_part = lax.rem(j, per_share)
    my_slot = i * per_share + my_part
    stays = to_share == my_share
    far = rows_y // 2
    order = ((0, 2), (1, 0), (1, 1), (1, 3), (0, 0), (0, 1), (0, 3), (1, 2))
    raw_copies = [
        pltpu.make_async_copy(array, raw.at[a], raw_sem.at[a]) for a, array in enumerate((field_modes, cotangent))
    ]
    table_copies = [
        pltpu.make_async_copy(source, target, table_sem.at[n])
        for n, (source, target) in enumerate(
            (
                (hartley_in, hartley),
                (lift_fields_in, lift_fields),
                (lift_adjoint_in, lift_adjoint),
                (lower_in, lower),
            )
        )
    ]
    for copy in raw_copies + table_copies:
        copy.start()
    tables = (lift_fields, lift_adjoint)

    def device(target):
        return {"kx": target // ncz, "cz": lax.rem(target, ncz)}

    def block(ref, slot):
        part = lax.rem(slot, per_share)
        rows = pl.ds(pl.multiple_of((slot // per_share) * local_m, local_m), local_m)
        columns = pl.ds(pl.multiple_of(part * local_k, local_k), local_k) if per_share > 1 else slice(None)
        return ref.at[rows, columns]

    def other(mine, step):
        half = jnp.where(step < far, 1 - mine // far, mine // far)
        return half * far + lax.rem(mine + 1 + step, far)

    def wait(ref, sem):
        pltpu.make_async_copy(ref, ref, sem).wait()

    def in_remote(h, y):
        return pltpu.make_async_remote_copy(
            src_ref=rows.at[h, y],
            dst_ref=block(held.at[h], my_slot),
            send_sem=in_send,
            recv_sem=in_recv.at[h],
            device_id=device(y * shares + to_share),
            device_id_type=MESH,
        )

    chunk = 128 if columns % 128 == 0 else columns

    for h, (a, f) in enumerate(order):
        if h < 2:
            raw_copies[h].wait()

        def turn(step, carry):
            here = pl.ds(pl.multiple_of(step * chunk, chunk), chunk)
            wide[here, :] = raw[a, :, f, here].astype(jnp.float32).T
            return carry

        lax.fori_loop(0, columns // chunk, turn, 0)
        for y in range(rows_y):
            rows[h, y] = wide[pl.ds(y, local_m, stride=rows_y), :].astype(jnp.bfloat16)

        def send(step, carry):
            in_remote(h, other(my_y, step)).start()
            return carry

        lax.fori_loop(0, rows_y - 1, send, 0)

        @pl.when(stays)
        def _():
            pltpu.make_async_copy(rows.at[h, my_y], block(held.at[h], my_slot), in_recv.at[h]).start()

        @pl.when(jnp.logical_not(stays))
        def _():
            in_remote(h, my_y).start()

    def share_rows(q):
        return pl.ds(pl.multiple_of(q * share_x, share_x), share_x)

    def mix(h):
        wait(held.at[h], in_recv.at[h])
        mixed[h] = matmul(hartley[...], held[h]).astype(jnp.bfloat16)
        for step in range(1, shares):
            q = lax.rem(my_share + step, shares)
            pltpu.make_async_remote_copy(
                src_ref=mixed.at[h, share_rows(q), :],
                dst_ref=halves.at[h, my_share],
                send_sem=swap_send,
                recv_sem=swap_recv.at[h],
                device_id=device(my_y * shares + q),
                device_id_type=MESH,
            ).start()
        pltpu.make_async_copy(
            mixed.at[h, share_rows(my_share), :], halves.at[h, my_share], swap_recv.at[h]
        ).start()

    block_z = 256 if points_z % 256 == 0 else points_z

    def lift(h, use):
        wait(halves.at[h], swap_recv.at[h])
        table = tables[order[h][0]]

        def one(step, carry):
            here = pl.ds(pl.multiple_of(step * block_z, block_z), block_z)
            value = matmul(halves[h, 0], table[0, :, here])
            for q in range(1, shares):
                value += matmul(halves[h, q], table[q, :, here])
            use(here, value)
            return carry

        lax.fori_loop(0, points_z // block_z, one, 0)

    def leave(f):
        for q in range(shares):
            lowered[f, q] = matmul(flux[...], lower[q]).astype(jnp.bfloat16)
        for step in range(1, shares):
            q = lax.rem(my_share + step, shares)
            pltpu.make_async_remote_copy(
                src_ref=lowered.at[f, q],
                dst_ref=turned.at[f, share_rows(my_share), :],
                send_sem=back_send,
                recv_sem=back_recv.at[f],
                device_id=device(my_y * shares + q),
                device_id_type=MESH,
            ).start()
        pltpu.make_async_copy(
            lowered.at[f, my_share], turned.at[f, share_rows(my_share), :], back_recv.at[f]
        ).start()

    def out_remote(f, slot):
        target = (slot // per_share) * ncz + my_share * per_share + lax.rem(slot, per_share)
        return pltpu.make_async_remote_copy(
            src_ref=block(result.at[f], slot),
            dst_ref=landed.at[f, my_y],
            send_sem=out_send,
            recv_sem=out_recv.at[f],
            device_id=device(target),
            device_id_type=MESH,
        )

    def finish(f):
        wait(turned.at[f], back_recv.at[f])
        result[f] = matmul(hartley[...], turned[f]).astype(jnp.bfloat16)

        def send(step, carry):
            out_remote(f, other(my_slot, step)).start()
            return carry

        lax.fori_loop(0, rows_y - 1, send, 0)

        @pl.when(stays)
        def _():
            pltpu.make_async_copy(block(result.at[f], my_slot), landed.at[f, my_y], out_recv.at[f]).start()

        @pl.when(jnp.logical_not(stays))
        def _():
            out_remote(f, my_slot).start()

    def keep(h):
        def use(here, value):
            points[h, :, here] = value
        return use

    def keep_and_flux(h):
        def use(here, value):
            points[h, :, here] = value
            flux[:, here] = (value * points[0, :, here]).astype(jnp.bfloat16)
        return use

    def first(here, value):
        total[:, here] = points[1, :, here] * value

    def add(h):
        def use(here, value):
            total[:, here] += points[h, :, here] * value
        return use

    def last(here, value):
        flux[:, here] = (total[:, here] + 2.0 * value * points[0, :, here]).astype(jnp.bfloat16)

    for copy in table_copies:
        copy.wait()
    mix(0)
    mix(1)
    lift(0, keep(0))
    lift(1, keep_and_flux(1))
    leave(0)
    mix(2)
    finish(0)
    lift(2, keep_and_flux(2))
    leave(1)
    mix(3)
    finish(1)
    lift(3, keep_and_flux(3))
    leave(3)
    mix(4)
    finish(3)
    lift(4, first)
    mix(5)
    lift(5, add(2))
    mix(6)
    lift(6, add(3))
    mix(7)
    lift(7, last)
    leave(2)
    finish(2)

    for f in (0, 1, 3, 2):
        wait(landed.at[f], out_recv.at[f])
        for y in range(rows_y):
            wide[pl.ds(y, local_m, stride=rows_y), :] = landed[f, y].astype(jnp.float32)

        def turn_back(step, carry):
            here = pl.ds(pl.multiple_of(step * chunk, chunk), chunk)
            out[f, :, here] = wide[here, :].T.astype(jnp.bfloat16)
            return carry

        lax.fori_loop(0, columns // chunk, turn_back, 0)

    @pl.when(stays)
    def _():
        wait(rows.at[:, pl.ds(0, rows_y - 1)], in_send)

    @pl.when(jnp.logical_not(stays))
    def _():
        wait(rows, in_send)

    if shares > 1:
        wait(mixed.at[:, pl.ds(0, share_x * (shares - 1)), :], swap_send)
        wait(lowered.at[:, pl.ds(0, shares - 1)], back_send)

    @pl.when(stays)
    def _():
        wait(landed.at[:, pl.ds(0, rows_y - 1)], out_send)

    @pl.when(jnp.logical_not(stays))
    def _():
        wait(landed, out_send)


def on_device(nkx, ncz, field_modes, cotangent):
    local_k, fields, columns = field_modes.shape
    local_m = columns // Y
    modes_z, points_x = local_k * ncz, local_m * nkx
    shares = nkx * ncz // Y
    group_k = modes_z // shares
    share_x = points_x // shares
    bf16 = jnp.bfloat16

    cosines = cosine_table(MZ, modes_z)
    synthesis = jnp.asarray((cosines * math.sqrt(2.0 / modes_z)).astype(bf16))
    projection = jnp.asarray((cosines * math.sqrt(2.0 / MZ)).astype(bf16))
    hartley = jnp.asarray(hartley_table(points_x).astype(np.float32).astype(bf16))
    lift_fields = synthesis.T.reshape(shares, group_k, MZ)
    lift_adjoint = projection.T.reshape(shares, group_k, MZ)
    lower = synthesis.reshape(MZ, shares, group_k).transpose(1, 0, 2)

    hbm = pl.BlockSpec(memory_space=pltpu.HBM)
    dma = pltpu.SemaphoreType.DMA
    out = pl.pallas_call(
        functools.partial(kernel, nkx, ncz, shares),
        out_shape=jax.ShapeDtypeStruct((fields, local_k, columns), bf16),
        in_specs=[hbm] * 6,
        out_specs=pl.BlockSpec(memory_space=pltpu.VMEM),
        scratch_shapes=[
            pltpu.VMEM((2, local_k, fields, columns), bf16),
            pltpu.VMEM(hartley.shape, bf16),
            pltpu.VMEM(lift_fields.shape, bf16),
            pltpu.VMEM(lift_adjoint.shape, bf16),
            pltpu.VMEM(lower.shape, bf16),
            dma((2,)), dma((4,)),
            pltpu.VMEM((columns, local_k), jnp.float32),
            pltpu.VMEM((2 * fields, Y, local_m, local_k), bf16),
            pltpu.VMEM((fields, Y, local_m, local_k), bf16),
            pltpu.VMEM((2 * fields, points_x, group_k), bf16),
            pltpu.VMEM((2 * fields, points_x, group_k), bf16),
            pltpu.VMEM((2 * fields, shares, share_x, group_k), bf16),
            pltpu.VMEM((fields, share_x, MZ), jnp.float32),
            pltpu.VMEM((share_x, MZ), jnp.float32),
            pltpu.VMEM((share_x, MZ), bf16),
            pltpu.VMEM((fields, shares, share_x, group_k), bf16),
            pltpu.VMEM((fields, points_x, group_k), bf16),
            pltpu.VMEM((fields, points_x, group_k), bf16),
            dma, dma((2 * fields,)), dma, dma((2 * fields,)),
            dma, dma((fields,)), dma, dma((fields,)),
        ],
        compiler_params=pltpu.CompilerParams(has_side_effects=True, vmem_limit_bytes=63 * 2**20),
    )(field_modes, cotangent, hartley, lift_fields, lift_adjoint, lower)
    return out.transpose(1, 0, 2)


def solution(mesh):
    return jax.shard_map(
        functools.partial(on_device, mesh.shape["kx"], mesh.shape["cz"]),
        mesh=mesh,
        in_specs=(P("cz", None, "kx"), P("cz", None, "kx")),
        out_specs=P("cz", None, "kx"),
        check_vma=False,
    )
```

```python
import functools
import math

import jax
import jax.numpy as jnp
import numpy as np
from jax import lax
from jax.experimental import pallas as pl
from jax.experimental.pallas import tpu as pltpu
from jax.sharding import PartitionSpec as P

MZ = 768
Y = 16
MESH = pl.DeviceIdType.MESH


def cosine_table(rows, columns):
    position = (np.arange(columns)[None, :] * (2 * np.arange(rows)[:, None] + 1)) % (4 * rows)
    return np.cos(np.pi * position / (2 * rows)).astype(np.float32)


def hartley_table(points):
    index = np.arange(points)
    phases = 2.0 * np.pi * ((index[:, None] * index[None, :]) % points) / points
    return (np.cos(phases) + np.sin(phases)) / math.sqrt(points)


def matmul(a, b):
    return jnp.dot(a, b, preferred_element_type=jnp.float32)


def kernel(
    nkx, ncz, shares,
    field_modes, cotangent, hartley_in, lift_fields_in, lift_adjoint_in, lower_in,
    out,
    raw, hartley, lift_fields, lift_adjoint, lower, raw_sem, table_sem,
    wide, rows, held, mixed, halves, points, total, flux, lowered, turned, result,
    in_send, in_recv, swap_send, swap_recv, back_send, back_recv, out_send, out_recv,
):
    local_k, fields, columns = field_modes.shape
    rows_y = rows.shape[1]
    local_m = columns // rows_y
    per_share = ncz // shares
    points_x = hartley.shape[0]
    points_z = lift_fields.shape[2]
    share_x = points_x // shares
    i, j = lax.axis_index("kx"), lax.axis_index("cz")
    linear = i * ncz + j
    my_y, my_share = linear // shares, lax.rem(linear, shares)
    to_share = j // per_share
    my_part = lax.rem(j, per_share)
    my_slot = i * per_share + my_part
    stays = to_share == my_share
    far = rows_y // 2
    order = ((0, 2), (1, 0), (1, 1), (1, 3), (0, 0), (0, 1), (0, 3), (1, 2))
    def device(target):
        return {"kx": target // ncz, "cz": lax.rem(target, ncz)}

    raw_copies = [
        pltpu.make_async_copy(array, raw.at[a], raw_sem.at[a]) for a, array in enumerate((field_modes, cotangent))
    ]
    table_copies = [
        pltpu.make_async_copy(source, target, table_sem.at[n])
        for n, (source, target) in enumerate(
            (
                (hartley_in, hartley),
                (lift_fields_in, lift_fields),
                (lift_adjoint_in, lift_adjoint),
                (lower_in, lower),
            )
        )
    ]
    for copy in raw_copies + table_copies:
        copy.start()
    barrier = pltpu.get_barrier_semaphore()

    def greet(step, carry):
        pl.semaphore_signal(
            barrier, inc=1, device_id=device(lax.rem(linear + step, nkx * ncz)), device_id_type=MESH
        )
        return carry

    lax.fori_loop(1, nkx * ncz, greet, 0)
    tables = (lift_fields, lift_adjoint)

    def block(ref, slot):
        part = lax.rem(slot, per_share)
        rows = pl.ds(pl.multiple_of((slot // per_share) * local_m, local_m), local_m)
        columns = pl.ds(pl.multiple_of(part * local_k, local_k), local_k) if per_share > 1 else slice(None)
        return ref.at[rows, columns]

    def other(mine, step):
        half = jnp.where(step < far, 1 - mine // far, mine // far)
        return half * far + lax.rem(mine + 1 + step, far)

    def wait(ref, sem):
        pltpu.make_async_copy(ref, ref, sem).wait()

    def in_remote(h, y):
        return pltpu.make_async_remote_copy(
            src_ref=rows.at[h, y],
            dst_ref=block(held.at[h], my_slot),
            send_sem=in_send,
            recv_sem=in_recv.at[h],
            device_id=device(y * shares + to_share),
            device_id_type=MESH,
        )

    chunk = 128 if columns % 128 == 0 else columns

    for h, (a, f) in enumerate(order):
        if h < 2:
            raw_copies[h].wait()

        def turn(step, carry):
            here = pl.ds(pl.multiple_of(step * chunk, chunk), chunk)
            wide[here, :] = raw[a, :, f, here].astype(jnp.float32).T
            return carry

        lax.fori_loop(0, columns // chunk, turn, 0)
        for y in range(rows_y):
            rows[h, y] = wide[pl.ds(y, local_m, stride=rows_y), :].astype(jnp.bfloat16)
        if h == 0:
            pl.semaphore_wait(barrier, nkx * ncz - 1)

        def send(step, carry):
            in_remote(h, other(my_y, step)).start()
            return carry

        lax.fori_loop(0, rows_y - 1, send, 0)

        @pl.when(stays)
        def _():
            pltpu.make_async_copy(rows.at[h, my_y], block(held.at[h], my_slot), in_recv.at[h]).start()

        @pl.when(jnp.logical_not(stays))
        def _():
            in_remote(h, my_y).start()

    def share_rows(q):
        return pl.ds(pl.multiple_of(q * share_x, share_x), share_x)

    def mix(h):
        wait(held.at[h], in_recv.at[h])
        mixed[h] = matmul(hartley[...], held[h]).astype(jnp.bfloat16)
        for step in range(1, shares):
            q = lax.rem(my_share + step, shares)
            pltpu.make_async_remote_copy(
                src_ref=mixed.at[h, share_rows(q), :],
                dst_ref=halves.at[h, my_share],
                send_sem=swap_send,
                recv_sem=swap_recv.at[h],
                device_id=device(my_y * shares + q),
                device_id_type=MESH,
            ).start()
        pltpu.make_async_copy(
            mixed.at[h, share_rows(my_share), :], halves.at[h, my_share], swap_recv.at[h]
        ).start()

    block_z = 256 if points_z % 256 == 0 else points_z

    def lift(h, use):
        wait(halves.at[h], swap_recv.at[h])
        table = tables[order[h][0]]

        def one(step, carry):
            here = pl.ds(pl.multiple_of(step * block_z, block_z), block_z)
            value = matmul(halves[h, 0], table[0, :, here])
            for q in range(1, shares):
                value += matmul(halves[h, q], table[q, :, here])
            use(here, value)
            return carry

        lax.fori_loop(0, points_z // block_z, one, 0)

    def leave(f):
        for q in range(shares):
            lowered[f, q] = matmul(flux[...], lower[q]).astype(jnp.bfloat16)
        for step in range(1, shares):
            q = lax.rem(my_share + step, shares)
            pltpu.make_async_remote_copy(
                src_ref=lowered.at[f, q],
                dst_ref=turned.at[f, share_rows(my_share), :],
                send_sem=back_send,
                recv_sem=back_recv.at[f],
                device_id=device(my_y * shares + q),
                device_id_type=MESH,
            ).start()
        pltpu.make_async_copy(
            lowered.at[f, my_share], turned.at[f, share_rows(my_share), :], back_recv.at[f]
        ).start()

    def out_remote(f, slot):
        target = (slot // per_share) * ncz + my_share * per_share + lax.rem(slot, per_share)
        return pltpu.make_async_remote_copy(
            src_ref=block(result.at[f], slot),
            dst_ref=out.at[my_y, f],
            send_sem=out_send,
            recv_sem=out_recv.at[f],
            device_id=device(target),
            device_id_type=MESH,
        )

    def finish(f):
        wait(turned.at[f], back_recv.at[f])
        result[f] = matmul(hartley[...], turned[f]).astype(jnp.bfloat16)

        def send(step, carry):
            out_remote(f, other(my_slot, step)).start()
            return carry

        lax.fori_loop(0, rows_y - 1, send, 0)

        @pl.when(stays)
        def _():
            pltpu.make_async_copy(block(result.at[f], my_slot), out.at[my_y, f], out_recv.at[f]).start()

        @pl.when(jnp.logical_not(stays))
        def _():
            out_remote(f, my_slot).start()

    def keep(h):
        def use(here, value):
            points[h, :, here] = value
        return use

    def keep_and_flux(h):
        def use(here, value):
            points[h, :, here] = value
            flux[:, here] = (value * points[0, :, here]).astype(jnp.bfloat16)
        return use

    def first(here, value):
        total[:, here] = points[1, :, here] * value

    def add(h):
        def use(here, value):
            total[:, here] += points[h, :, here] * value
        return use

    def last(here, value):
        flux[:, here] = (total[:, here] + 2.0 * value * points[0, :, here]).astype(jnp.bfloat16)

    for copy in table_copies:
        copy.wait()
    mix(0)
    mix(1)
    lift(0, keep(0))
    lift(1, keep_and_flux(1))
    leave(0)
    mix(2)
    finish(0)
    lift(2, keep_and_flux(2))
    leave(1)
    mix(3)
    finish(1)
    lift(3, keep_and_flux(3))
    leave(3)
    mix(4)
    finish(3)
    lift(4, first)
    mix(5)
    lift(5, add(2))
    mix(6)
    lift(6, add(3))
    mix(7)
    lift(7, last)
    leave(2)
    finish(2)

    @pl.when(stays)
    def _():
        wait(rows.at[:, pl.ds(0, rows_y - 1)], in_send)

    @pl.when(jnp.logical_not(stays))
    def _():
        wait(rows, in_send)

    if shares > 1:
        wait(mixed.at[:, pl.ds(0, share_x * (shares - 1)), :], swap_send)
        wait(lowered.at[:, pl.ds(0, shares - 1)], back_send)

    @pl.when(stays)
    def _():
        wait(out.at[pl.ds(0, rows_y - 1)], out_send)

    @pl.when(jnp.logical_not(stays))
    def _():
        wait(out, out_send)

    for f in range(fields):
        wait(out.at[:, f], out_recv.at[f])


def on_device(nkx, ncz, field_modes, cotangent):
    local_k, fields, columns = field_modes.shape
    local_m = columns // Y
    modes_z, points_x = local_k * ncz, local_m * nkx
    shares = nkx * ncz // Y
    group_k = modes_z // shares
    share_x = points_x // shares
    bf16 = jnp.bfloat16

    cosines = cosine_table(MZ, modes_z)
    synthesis = jnp.asarray((cosines * math.sqrt(2.0 / modes_z)).astype(bf16))
    projection = jnp.asarray((cosines * math.sqrt(2.0 / MZ)).astype(bf16))
    hartley = jnp.asarray(hartley_table(points_x).astype(np.float32).astype(bf16))
    lift_fields = synthesis.T.reshape(shares, group_k, MZ)
    lift_adjoint = projection.T.reshape(shares, group_k, MZ)
    lower = synthesis.reshape(MZ, shares, group_k).transpose(1, 0, 2)

    hbm = pl.BlockSpec(memory_space=pltpu.HBM)
    dma = pltpu.SemaphoreType.DMA
    out = pl.pallas_call(
        functools.partial(kernel, nkx, ncz, shares),
        out_shape=jax.ShapeDtypeStruct((Y, fields, local_m, local_k), bf16),
        in_specs=[hbm] * 6,
        out_specs=pl.BlockSpec(memory_space=pl.ANY),
        scratch_shapes=[
            pltpu.VMEM((2, local_k, fields, columns), bf16),
            pltpu.VMEM(hartley.shape, bf16),
            pltpu.VMEM(lift_fields.shape, bf16),
            pltpu.VMEM(lift_adjoint.shape, bf16),
            pltpu.VMEM(lower.shape, bf16),
            dma((2,)), dma((4,)),
            pltpu.VMEM((columns, local_k), jnp.float32),
            pltpu.VMEM((2 * fields, Y, local_m, local_k), bf16),
            pltpu.VMEM((2 * fields, points_x, group_k), bf16),
            pltpu.VMEM((2 * fields, points_x, group_k), bf16),
            pltpu.VMEM((2 * fields, shares, share_x, group_k), bf16),
            pltpu.VMEM((fields, share_x, MZ), jnp.float32),
            pltpu.VMEM((share_x, MZ), jnp.float32),
            pltpu.VMEM((share_x, MZ), bf16),
            pltpu.VMEM((fields, shares, share_x, group_k), bf16),
            pltpu.VMEM((fields, points_x, group_k), bf16),
            pltpu.VMEM((fields, points_x, group_k), bf16),
            dma, dma((2 * fields,)), dma, dma((2 * fields,)),
            dma, dma((fields,)), dma, dma((fields,)),
        ],
        compiler_params=pltpu.CompilerParams(has_side_effects=True, vmem_limit_bytes=63 * 2**20, collective_id=0),
    )(field_modes, cotangent, hartley, lift_fields, lift_adjoint, lower)
    return out.transpose(3, 1, 2, 0).reshape(local_k, fields, columns)


def solution(mesh):
    return jax.shard_map(
        functools.partial(on_device, mesh.shape["kx"], mesh.shape["cz"]),
        mesh=mesh,
        in_specs=(P("cz", None, "kx"), P("cz", None, "kx")),
        out_specs=P("cz", None, "kx"),
        check_vma=False,
    )
```
